32 devices in a mesh: batch: 8 (over z, y), vocab: 4 (over x, core).
Axes of the slice: x: 2, y: 2, z: 4, core: 2. Of those that a mesh axis runs over, the one named last changes fastest.
Arguments:
- hidden: bfloat16 [4096, 3584], P(('batch', 'vocab')), may hold values from -6 to 6
- head_weight: bfloat16 [3072, 3584], P('vocab', 'batch'), may hold values from -0.3125 to 0.3125
- targets: int32 [4096], P(('batch', 'vocab')), may hold values from 0 to 3071
- valid_mask: int32 [4096], P(('batch', 'vocab')), may hold values 0 or 1
Outputs:
- head_grad: float32 [3072, 3584], P('vocab', 'batch')
- hidden_grad: float32 [4096, 3584], P(('batch', 'vocab'))
- mean_loss: float32 [], replicated
The draws below stay inside these ranges and needn't reach their ends.
All inputs are finite; a program needn't handle non-finite values. No bound on the sum of `valid_mask` on one device may be relied on, other than what follows from the above.
Results may differ from the reference program's by a relative error of at most 0.0019.
Values may be sent and summed in bfloat16 or wider, within the bound.
A program may use at most 128 MiB of HBM per device.

```python
import jax
import jax.numpy as jnp
from jax import lax

D = 3584
GROUP_TOK = 512
TOKENS = 4096
VOCAB = 3072
N_BATCH = 8


def set_ends(drawn, stream_key, smallest, top_value):
    spot = [jax.random.randint(jax.random.fold_in(stream_key, axis), (), 0, length) for axis, length in enumerate(drawn.shape)]
    longest = drawn.shape.index(max(drawn.shape))
    neighbour = spot[:longest] + [(spot[longest] + 1) % drawn.shape[longest]] + spot[longest + 1:]
    return drawn.at[tuple(spot)].set(smallest).at[tuple(neighbour)].set(top_value)


def steps_of(rng, dims, split, low, high):
    def one(axis_at, parts):
        steps = jax.random.uniform(jax.random.fold_in(jax.random.fold_in(rng, 6), axis_at), (parts,), jnp.float32, low / len(split), high / len(split))
        return jnp.repeat(jnp.exp(steps), dims[axis_at] // parts).reshape((-1,) + (1,) * (len(dims) - axis_at - 1))

    gain = one(*split[0])
    for cut in split[1:]:
        gain = gain * one(*cut)
    return gain


def normal_values(stream_key, dims, scale, most, shards=(), held_as=jnp.bfloat16):
    factor_of = steps_of(stream_key, dims, shards, -0.22, 0.18) if shards else 1.0
    array = jax.random.normal(stream_key, dims, jnp.float32) * scale * factor_of
    return jnp.minimum(jnp.maximum(array, -most), most).astype(held_as)


def setup_inputs(seed: int = 0) -> dict:
    arg_keys = jax.random.split(jax.random.key(seed), 5)
    hidden = normal_values(arg_keys[0], (TOKENS, D), 1.0, 6.0, ((0, 32),))
    head_weight = normal_values(arg_keys[1], (VOCAB, D), (D // 9) ** -0.5, 0.3125, ((0, 4), (1, 8)))
    targets = set_ends(jax.random.randint(arg_keys[2], (TOKENS,), 0, VOCAB), jax.random.fold_in(arg_keys[2], 1), 0, VOCAB - 1).astype(jnp.int32)
    valid_mask = set_ends((jax.random.randint(arg_keys[3], (TOKENS,), 0, 4) < 3).astype(jnp.int32), jax.random.fold_in(arg_keys[3], 1), 0, 1)
    return {"hidden": hidden, "head_weight": head_weight, "targets": targets, "valid_mask": valid_mask}


softcap = 30.0


def reference(hidden, head_weight, targets, valid_mask):
    positions = hidden.shape[0]
    model_width = hidden.shape[1]
    state_blocks = hidden.reshape(N_BATCH, GROUP_TOK, model_width)
    target_blocks = targets.reshape(N_BATCH, GROUP_TOK)
    mask_blocks = valid_mask.reshape(N_BATCH, GROUP_TOK)
    vocab_ids = jnp.arange(VOCAB, dtype=jnp.int32)

    def token_block(running, scanned):
        grad_total, loss_total = running
        row_block, target_ids, mask_block = scanned
        scores = lax.dot_general(row_block, head_weight, (((1,), (1,)), ((), ())), preferred_element_type=jnp.float32)
        logits = softcap * jnp.tanh(scores / softcap)
        target_hit = vocab_ids[None, :] == target_ids[:, None]
        exponent = jnp.exp(logits)
        partition = jnp.sum(exponent, axis=1)
        target_logit = jnp.sum(jnp.where(target_hit, logits, 0.0), axis=1)
        weight = mask_block.astype(jnp.float32)
        slope = 1.0 - (logits / softcap) ** 2
        delta_logit = (weight[:, None] * (exponent / partition[:, None] - target_hit.astype(jnp.float32)) * slope).astype(jnp.bfloat16)
        grad_total = grad_total + lax.dot_general(delta_logit, row_block, (((0,), (0,)), ((), ())), preferred_element_type=jnp.float32)
        loss_total = loss_total + jnp.sum(weight * (jnp.log(partition) - target_logit))
        state_grad = jnp.dot(delta_logit, head_weight, preferred_element_type=jnp.float32)
        return (grad_total, loss_total), state_grad

    start_grad = jnp.zeros(head_weight.shape, jnp.float32)
    start_loss = jnp.zeros((), jnp.float32)
    (head_grad, loss_total), state_grads = lax.scan(token_block, (start_grad, start_loss), (state_blocks, target_blocks, mask_blocks))
    hidden_grad = state_grads.reshape(positions, model_width)
    mean_loss = loss_total / positions
    return head_grad, hidden_grad, mean_loss
```

```python
import functools

import jax
import jax.numpy as jnp
from jax import lax
from jax.experimental import pallas as pl
from jax.experimental.pallas import tpu as pltpu
from jax.sharding import PartitionSpec as P

softcap = 30.0
MESH = pl.DeviceIdType.MESH
f32, bf16 = jnp.float32, jnp.bfloat16


def chunk_of(length, most):
    return max(s for s in range(16, most + 1, 16) if length % s == 0)


def kernel(sizes, h_in, w_in, code_in, head_out, hid_out, loss_out, h_all, w_all, code_all,
           logits, delta, stat_own, stat_all, loss_own, loss_all, grad, grad_send, y_in, z_out, z_in,
           part, core_in, x_out, x_in, *sems):
    nz, ny, nx, nv = sizes
    (own_sem, hs, hd, hr, ws_up, ws_dn, ws_y, wr, cs, cr, ss, sr, ls, lr,
     ys, yr, zs, zr, ds, dr, xs, xr) = sems
    nb = nz * ny
    rows, width = h_in.shape
    cols, entries = w_in.shape
    tokens = rows * nv
    b, v = lax.axis_index("batch"), lax.axis_index("vocab")
    z, y = lax.div(b, ny), lax.rem(b, ny)
    x, core = lax.div(v, 2), lax.rem(v, 2)
    other = x * 2 + 1 - core

    def at(bb, vv):
        return {"batch": bb, "vocab": vv}

    def copy(src, dst, send, recv, bb, vv):
        return pltpu.make_async_remote_copy(
            src_ref=src, dst_ref=dst, send_sem=send, recv_sem=recv, device_id=at(bb, vv), device_id_type=MESH)

    def hrow(i):
        return pl.ds(pl.multiple_of(i * rows, 16), rows)

    def wrow(i):
        return pl.ds(pl.multiple_of(i * cols, 16), cols)

    barrier = pltpu.get_barrier_semaphore()
    for k in range(1, nb):
        pl.semaphore_signal(barrier, inc=1, device_id=at(lax.rem(b + k, nb), v), device_id_type=MESH)
    for k in range(1, nv):
        pl.semaphore_signal(barrier, inc=1, device_id=at(b, lax.rem(v + k, nv)), device_id_type=MESH)
    pl.semaphore_wait(barrier, nb - 1 + nv - 1)

    def w_copy(zz, kind, k=0):
        i = zz * ny + y
        dst = w_all.at[wrow(i)]
        if kind == "up":
            return copy(dst, dst, ws_up.at[zz], wr.at[i], (z + 1) * ny + y, v)
        if kind == "down":
            return copy(dst, dst, ws_dn.at[zz], wr.at[i], (z - 1) * ny + y, v)
        return copy(dst, dst, ws_y.at[k - 1, zz], wr.at[i], z * ny + lax.rem(y + k, ny), v)

    def w_own(kind, k=0):
        dst = w_all.at[wrow(b)]
        if kind == "up":
            return copy(w_in, dst, ws_up.at[z], wr.at[b], b + ny, v)
        if kind == "down":
            return copy(w_in, dst, ws_dn.at[z], wr.at[b], b - ny, v)
        return copy(w_in, dst, ws_y.at[k - 1, z], wr.at[b], z * ny + lax.rem(y + k, ny), v)

    def h_x(k):
        return copy(h_in, h_all.at[hrow(v)], hs.at[k - 1], hr.at[v], b, lax.rem(x + k, nx) * 2 + core)

    def h_core(xx, own=False):
        i = xx * 2 + core
        dst = h_all.at[hrow(i)]
        return copy(h_in if own else dst, dst, hd.at[xx], hr.at[i], b, other)

    def code_copy(k):
        return copy(code_in, code_all.at[hrow(v)], cs.at[k - 1], cr.at[v], b, lax.rem(v + k, nv))

    for k in range(1, nv):
        code_copy(k).start()
    has_up, has_down = z + 1 < nz, z >= 1
    pl.when(has_up)(lambda: w_own("up").start())
    pl.when(has_down)(lambda: w_own("down").start())
    for k in range(1, ny):
        w_own("y", k).start()
    for k in range(1, nx):
        h_x(k).start()
    h_core(x, True).start()
    local = [
        pltpu.make_async_copy(w_in, w_all.at[wrow(b)], own_sem.at[0]),
        pltpu.make_async_copy(h_in, h_all.at[hrow(v)], own_sem.at[1]),
        pltpu.make_async_copy(code_in, code_all.at[hrow(v)], own_sem.at[2]),
    ]
    for one in local:
        one.start()

    for k in range(1, nz):
        @pl.when(z - k >= 0)
        def _():
            w_copy(z - k, "up").wait_recv()
            pl.when(has_up)(lambda: w_copy(z - k, "up").start())
            for j in range(1, ny):
                w_copy(z - k, "y", j).start()

        @pl.when(z + k < nz)
        def _():
            w_copy(z + k, "down").wait_recv()
            pl.when(has_down)(lambda: w_copy(z + k, "down").start())
            for j in range(1, ny):
                w_copy(z + k, "y", j).start()

        if k == 1:
            for j in range(1, nx):
                xx = lax.rem(x + j, nx)
                h_core(xx).wait_recv()
                h_core(xx).start()

    for one in local:
        one.wait()
    for j in range(nx):
        xx = lax.rem(x + j, nx)
        i = xx * 2 + 1 - core
        copy(h_in, h_all.at[hrow(i)], hd.at[xx], hr.at[i], b, other).wait_recv()
    for k in range(1, nv):
        i = lax.rem(v + k, nv)
        copy(code_in, code_all.at[hrow(i)], cs.at[k - 1], cr.at[i], b, i).wait_recv()
    for k in range(1, ny):
        yy = lax.rem(y + k, ny)
        for zz in range(nz):
            i = zz * ny + yy
            copy(w_in, w_all.at[wrow(i)], ws_y.at[k - 1, zz], wr.at[i], z * ny + yy, v).wait_recv()

    step = chunk_of(entries, 256)
    code = code_all[:, 0:1]
    weight = (code >= 0).astype(f32)

    def hits(n):
        ids = lax.broadcasted_iota(jnp.int32, (tokens, step), 1) + (v * entries + n * step)
        return ids == code

    def score_step(n, sums):
        total, hit_sum = sums
        span = pl.ds(pl.multiple_of(n * step, step), step)
        scores = jnp.dot(h_all[...], w_all[:, span], preferred_element_type=f32)
        capped = softcap * jnp.tanh(scores * (1.0 / softcap))
        logits[:, span] = capped
        total = total + jnp.sum(jnp.exp(capped), axis=1, keepdims=True)
        hit_sum = hit_sum + jnp.sum(jnp.where(hits(n), capped, 0.0), axis=1, keepdims=True)
        return total, hit_sum

    zero = jnp.zeros((tokens, 1), f32)
    total, hit_sum = lax.fori_loop(0, entries // step, score_step, (zero, zero))
    lane = lax.broadcasted_iota(jnp.int32, (tokens, 128), 1)
    turned = jnp.transpose(jnp.where(lane < 64, total, hit_sum))
    stat_own[...] = turned[56:72]

    def stat_copy(k):
        return copy(stat_own, stat_all.at[v], ss.at[k - 1], sr.at[v], b, lax.rem(v + k, nv))

    for k in range(1, nv):
        stat_copy(k).start()
    for k in range(1, nv):
        i = lax.rem(v + k, nv)
        copy(stat_own, stat_all.at[i], ss.at[k - 1], sr.at[i], b, i).wait_recv()
    stats = stat_own[...]
    for k in range(1, nv):
        stats = stats + stat_all[lax.rem(v + k, nv)]
    back = jnp.transpose(jnp.concatenate([stats[0:8]] * 8 + [stats[8:16]] * 8, axis=0))
    partition, target_logit = back[:, 0:1], back[:, 64:65]
    loss = jnp.sum(weight * (jnp.log(partition) - target_logit), axis=0, keepdims=True)
    loss_own[...] = jnp.broadcast_to(loss, loss_own.shape)

    def loss_copy(k):
        return copy(loss_own, loss_all.at[b], ls.at[k - 1], lr.at[b], lax.rem(b + k, nb), v)

    for k in range(1, nb):
        loss_copy(k).start()
    scale = weight / partition

    def delta_step(n, carry):
        span = pl.ds(pl.multiple_of(n * step, step), step)
        capped = logits[:, span]
        slope = 1.0 - (capped * (1.0 / softcap)) ** 2
        delta[:, span] = ((jnp.exp(capped) * scale - jnp.where(hits(n), weight, 0.0)) * slope).astype(bf16)
        return carry

    lax.fori_loop(0, entries // step, delta_step, 0)

    wide = chunk_of(width, 256)

    def grad_step(j, carry):
        span = pl.ds(pl.multiple_of(j * wide, wide), wide)
        share = lax.dot_general(h_all[:, span], delta[...], (((0,), (0,)), ((), ())), preferred_element_type=f32)
        grad[span, :] = share
        if grad_send is not None:
            grad_send[span, :] = share.astype(bf16)
        return carry

    lax.fori_loop(0, width // wide, grad_step, 0)
    y_src = grad if grad_send is None else grad_send

    def y_copy(k, zz):
        yy = lax.rem(y + k, ny)
        return copy(y_src.at[wrow(zz * ny + yy)], y_in.at[k - 1, zz], ys.at[k - 1, zz], yr.at[k - 1, zz],
                    z * ny + yy, v)

    order = [lax.rem(z + k, nz) for k in range(1, nz)] + [z]
    for zz in order:
        for k in range(1, ny):
            y_copy(k, zz).start()

    def part_step(j, carry):
        span = pl.ds(pl.multiple_of(j * wide, wide), wide)
        part[:, span] = lax.dot_general(
            delta[...], w_all[span, :], (((1,), (1,)), ((), ())), preferred_element_type=f32)
        return carry

    lax.fori_loop(0, width // wide, part_step, 0)

    def core_copy(xx):
        return copy(part.at[hrow(xx * 2 + 1 - core)], core_in.at[xx], ds.at[xx], dr.at[xx], b, other)

    def x_copy(k):
        return copy(x_out.at[k - 1], x_in.at[k - 1], xs.at[k - 1], xr.at[k - 1], b, lax.rem(x + k, nx) * 2 + core)

    xorder = [lax.rem(x + k, nx) for k in range(1, nx)] + [x]
    for xx in xorder:
        core_copy(xx).start()
    hstep = 16
    for k in range(1, nx + 1):
        xx = xorder[k - 1]
        core_copy(xx).wait_recv()

        def core_sum(r, carry):
            span = pl.ds(pl.multiple_of(r * hstep, hstep), hstep)
            mine = pl.ds(pl.multiple_of((xx * 2 + core) * rows + r * hstep, hstep), hstep)
            both = part[mine, :] + core_in[xx, span, :]
            if k < nx:
                x_out[k - 1, span, :] = both.astype(bf16)
            else:
                hid_out[span, :] = both
            return carry

        lax.fori_loop(0, rows // hstep, core_sum, 0)
        if k < nx:
            x_copy(k).start()

    cstep = chunk_of(cols, 64)

    def z_copy(k):
        zz = lax.rem(z + k, nz)
        return copy(z_out.at[k - 1], z_in.at[k - 1], zs.at[k - 1], zr.at[k - 1], zz * ny + y, v)

    for k in range(1, nz + 1):
        zz = order[k - 1]
        for j in range(1, ny):
            y_copy(j, zz).wait_recv()

        def y_sum(r, carry):
            span = pl.ds(pl.multiple_of(r * cstep, 16), cstep)
            total = grad[pl.ds(pl.multiple_of((zz * ny + y) * cols + r * cstep, 16), cstep), :]
            for j in range(1, ny):
                total = total + y_in[j - 1, zz, span, :].astype(f32)
            if k < nz:
                z_out[k - 1, span, :] = total.astype(bf16)
            else:
                head_out[span, :] = total
            return carry

        lax.fori_loop(0, cols // cstep, y_sum, 0)
        if k < nz:
            z_copy(k).start()

    for k in range(1, nx):
        x_copy(k).wait_recv()

        def x_sum(r, carry):
            span = pl.ds(pl.multiple_of(r * hstep, hstep), hstep)
            hid_out[span, :] += x_in[k - 1, span, :].astype(f32)
            return carry

        lax.fori_loop(0, rows // hstep, x_sum, 0)

    losses = loss_own[...]
    for k in range(1, nb):
        i = lax.rem(b + k, nb)
        copy(loss_own, loss_all.at[i], ls.at[k - 1], lr.at[i], i, v).wait_recv()
        losses = losses + loss_all[i]
    loss_out[...] = losses * (1.0 / (tokens * nb))

    for k in range(1, nz):
        z_copy(k).wait_recv()

        def z_sum(r, carry):
            span = pl.ds(pl.multiple_of(r * cstep, 16), cstep)
            head_out[span, :] += z_in[k - 1, span, :].astype(f32)
            return carry

        lax.fori_loop(0, cols // cstep, z_sum, 0)

    pl.when(has_up)(lambda: w_own("up").wait_send())
    pl.when(has_down)(lambda: w_own("down").wait_send())
    for k in range(1, ny):
        w_own("y", k).wait_send()
    for k in range(1, nz):
        @pl.when(z - k >= 0)
        def _():
            pl.when(has_up)(lambda: w_copy(z - k, "up").wait_send())
            for j in range(1, ny):
                w_copy(z - k, "y", j).wait_send()

        @pl.when(z + k < nz)
        def _():
            pl.when(has_down)(lambda: w_copy(z + k, "down").wait_send())
            for j in range(1, ny):
                w_copy(z + k, "y", j).wait_send()
        z_copy(k).wait_send()
    for k in range(1, nx):
        h_x(k).wait_send()
        h_core(lax.rem(x + k, nx)).wait_send()
        x_copy(k).wait_send()
    h_core(x, True).wait_send()
    for k in range(1, nv):
        code_copy(k).wait_send()
        stat_copy(k).wait_send()
    for k in range(1, nb):
        loss_copy(k).wait_send()
    for zz in order:
        for k in range(1, ny):
            y_copy(k, zz).wait_send()
    for xx in xorder:
        core_copy(xx).wait_send()


def local(nb, nv, hidden, head_weight, targets, valid_mask):
    nx = nv // 2
    ny = nx if nb % nx == 0 else 1
    nz = nb // ny
    rows, width = hidden.shape
    entries, cols = head_weight.shape
    tokens = rows * nv
    code = jnp.broadcast_to(jnp.where(valid_mask != 0, targets, -1)[:, None], (rows, 128))
    vm = pltpu.VMEM
    two = ny <= 2
    y_type = bf16 if two else f32
    dma = pltpu.SemaphoreType.DMA

    def some(n):
        return max(n, 1)

    buffers = [
        vm((tokens, width), bf16), vm((width, entries), bf16), vm((tokens, 128), jnp.int32),
        vm((tokens, entries), f32), vm((tokens, entries), bf16),
        vm((16, tokens), f32), vm((nv, 16, tokens), f32), vm((8, 128), f32), vm((nb, 8, 128), f32),
        vm((width, entries), f32), vm((width, entries) if two else (16, 128), bf16),
        vm((some(ny - 1), nz, cols, entries), y_type),
        vm((some(nz - 1), cols, entries), bf16), vm((some(nz - 1), cols, entries), bf16),
        vm((tokens, width), f32), vm((nx, rows, width), f32),
        vm((some(nx - 1), rows, width), bf16), vm((some(nx - 1), rows, width), bf16),
    ]
    sems = [
        dma((3,)), dma((some(nx - 1),)), dma((nx,)), dma((nv,)), dma((nz,)), dma((nz,)),
        dma((some(ny - 1), nz)), dma((nb,)), dma((nv,)), dma((nv,)), dma((nv,)), dma((nv,)), dma((nb,)), dma((nb,)),
        dma((some(ny - 1), nz)), dma((some(ny - 1), nz)), dma((nz,)), dma((nz,)), dma((nx,)), dma((nx,)),
        dma((nx,)), dma((nx,)),
    ]

    def body(*refs):
        refs = list(refs)
        if not two:
            refs[6 + 10] = None
        kernel((nz, ny, nx, nv), *refs)

    whole = pl.BlockSpec(memory_space=vm)
    head_t, hidden_grad, loss = pl.pallas_call(
        body,
        out_shape=(
            jax.ShapeDtypeStruct((cols, entries), f32),
            jax.ShapeDtypeStruct((rows, width), f32),
            jax.ShapeDtypeStruct((8, 128), f32),
        ),
        in_specs=[whole] * 3,
        out_specs=(whole,) * 3,
        scratch_shapes=buffers + sems,
        compiler_params=pltpu.CompilerParams(
            collective_id=0, has_side_effects=True, vmem_limit_bytes=67043328),
    )(hidden, jnp.transpose(head_weight), code)
    return jnp.transpose(head_t), hidden_grad, loss[0, 0]


def solution(mesh):
    placed = (
        P(("batch", "vocab"), None),
        P("vocab", "batch"),
        P(("batch", "vocab")),
        P(("batch", "vocab")),
    )
    return jax.shard_map(
        functools.partial(local, mesh.shape["batch"], mesh.shape["vocab"]),
        mesh=mesh,
        in_specs=placed,
        out_specs=(P("vocab", "batch"), P(("batch", "vocab"), None), P()),
        check_vma=False,
    )
```

```python
import functools

import jax
import jax.numpy as jnp
from jax import lax
from jax.experimental import pallas as pl
from jax.experimental.pallas import tpu as pltpu
from jax.sharding import PartitionSpec as P

softcap = 30.0
MESH = pl.DeviceIdType.MESH
f32, bf16 = jnp.float32, jnp.bfloat16


def chunk_of(length, most):
    return max(s for s in range(16, most + 1, 16) if length % s == 0)


def kernel(sizes, h_in, w_in, code_in, head_out, hid_out, loss_out, h_all, w_all, code_got, code_all,
           logits, delta, stat_own, stat_all, loss_own, loss_all, grad, grad_send, r_in,
           part, core_in, x_out, x_in, y_out, y_in, *sems):
    nz, ny, nx, nv = sizes
    (own_sem, hs, hf, hd, hr, ws_up, ws_dn, ws_y, wr, cs, cr, ss, sr, ls, lr,
     rs, rr, ds, dr, xs, xr, ys, yr) = sems
    nb = nz * ny
    rows, width = h_in.shape
    cols, half = w_in.shape[1:]
    group = ny * nv
    tokens = rows * group
    entries = ny * half
    b, v = lax.axis_index("batch"), lax.axis_index("vocab")
    z, y = lax.div(b, ny), lax.rem(b, ny)
    x, core = lax.div(v, 2), lax.rem(v, 2)
    other = x * 2 + 1 - core
    me = y * nv + v

    def at(bb, vv):
        return {"batch": bb, "vocab": vv}

    def copy(src, dst, send, recv, bb, vv):
        return pltpu.make_async_remote_copy(
            src_ref=src, dst_ref=dst, send_sem=send, recv_sem=recv, device_id=at(bb, vv), device_id_type=MESH)

    def hrow(i):
        return pl.ds(pl.multiple_of(i * rows, 16), rows)

    def wrow(i):
        return pl.ds(pl.multiple_of(i * cols, 16), cols)

    def turn_y(k):
        return lax.rem(y + k, ny)

    def turn_x(k):
        return lax.rem(x + k, nx)

    peers = [(k, j) for k in range(ny) for j in range(nv) if k or j]

    def peer(n):
        k, j = peers[n]
        return z * ny + turn_y(k), lax.rem(v + j, nv), turn_y(k) * nv + lax.rem(v + j, nv)

    barrier = pltpu.get_barrier_semaphore()
    for k in range(1, nb):
        pl.semaphore_signal(barrier, inc=1, device_id=at(lax.rem(b + k, nb), v), device_id_type=MESH)
    met = [n for n in range(len(peers)) if peers[n][1]]
    for n in met:
        bb, vv, _ = peer(n)
        pl.semaphore_signal(barrier, inc=1, device_id=at(bb, vv), device_id_type=MESH)
    pl.semaphore_wait(barrier, nb - 1 + len(met))

    def w_z(zz, yy, up, own=False):
        i = zz * ny + yy
        dst = w_all.at[wrow(i)]
        sem = (ws_up if up else ws_dn).at[i]
        return copy(w_in.at[y] if own else dst, dst, sem, wr.at[i], b + ny if up else b - ny, v)

    def w_y(k):
        return copy(w_in.at[turn_y(k)], w_all.at[wrow(b)], ws_y.at[k - 1], wr.at[b], z * ny + turn_y(k), v)

    def w_got(zz, yy):
        w_z(zz, yy, True).wait_recv()

    has_up, has_down = z + 1 < nz, z >= 1

    def h_send(n_src, sem, bb, vv, own=False):
        dst = h_all.at[hrow(n_src)]
        return copy(h_in if own else dst, dst, sem, hr.at[n_src], bb, vv)

    def h_x(k):
        return h_send(me, hs.at[k - 1], b, turn_x(k) * 2 + core, True)

    def h_y(k):
        return h_send(me, hs.at[nx + k - 1], z * ny + turn_y(k), v, True)

    def h_xy(kx, ky):
        return h_send(y * nv + turn_x(kx) * 2 + core, hf.at[kx, ky], z * ny + turn_y(ky), v)

    def h_yx(kx, ky):
        return h_send(turn_y(ky) * nv + v, hf.at[kx, ky], b, turn_x(kx) * 2 + core)

    def h_core(kx, ky):
        i = turn_y(ky) * nv + turn_x(kx) * 2 + core
        return h_send(i, hd.at[kx, ky], b, other, kx == 0 and ky == 0)

    def h_got(kx, ky, cc):
        i = turn_y(ky) * nv + turn_x(kx) * 2 + cc
        h_send(i, hd.at[kx, ky], b, other).wait_recv()

    def code_copy(n):
        bb, vv, _ = peer(n)
        return copy(code_in, code_got.at[me], cs.at[n], cr.at[me], bb, vv)

    for k in range(1, ny):
        w_y(k).start()
    pl.when(has_up)(lambda: w_z(z, y, True, True).start())
    pl.when(has_down)(lambda: w_z(z, y, False, True).start())
    for k in range(1, nx):
        h_x(k).start()
    for k in range(1, ny):
        h_y(k).start()
    for n in range(len(peers)):
        code_copy(n).start()
    h_core(0, 0).start()
    local = [
        pltpu.make_async_copy(w_in.at[y], w_all.at[wrow(b)], own_sem.at[0]),
        pltpu.make_async_copy(h_in, h_all.at[hrow(me)], own_sem.at[1]),
    ]
    for one in local:
        one.start()

    for k in range(1, ny):
        w_got(z, turn_y(k))
        pl.when(has_up)(lambda: w_z(z, turn_y(k), True).start())
        pl.when(has_down)(lambda: w_z(z, turn_y(k), False).start())

    def h_pass():
        for kx in range(1, nx):
            h_got(kx, 0, core)
            for ky in range(1, ny):
                pl.when(core == 0)(lambda: h_xy(kx, ky).start())
            h_core(kx, 0).start()
        for ky in range(1, ny):
            h_got(0, ky, core)
            for kx in range(1, nx):
                pl.when(core == 1)(lambda: h_yx(kx, ky).start())
            h_core(0, ky).start()

    def h_rest():
        for kx in range(1, nx):
            for ky in range(1, ny):
                h_got(kx, ky, core)
                h_core(kx, ky).start()

    for k in range(1, nz):
        for j in range(ny):
            yy = turn_y(j)

            @pl.when(z - k >= 0)
            def _():
                w_got(z - k, yy)
                pl.when(has_up)(lambda: w_z(z - k, yy, True).start())

            @pl.when(z + k < nz)
            def _():
                w_got(z + k, yy)
                pl.when(has_down)(lambda: w_z(z + k, yy, False).start())
        if k == 1:
            h_pass()
        if k == min(2, nz - 1):
            h_rest()

    for one in local:
        one.wait()
    for kx in range(nx):
        for ky in range(ny):
            h_got(kx, ky, 1 - core)
    code_got[me] = code_in[...]
    for n in range(len(peers)):
        bb, vv, i = peer(n)
        copy(code_in, code_got.at[i], cs.at[n], cr.at[i], bb, vv).wait_recv()
    for i in range(group):
        code_all[i * rows:(i + 1) * rows, :] = jnp.transpose(jnp.concatenate([code_got[i]] * 16, axis=0))

    step = chunk_of(tokens, 256)
    lanes = lax.broadcasted_iota(jnp.int32, (step, 128), 1)
    first = v * entries + y * half

    def span_of(n):
        return pl.ds(pl.multiple_of(n * step, step), step)

    def hits(n):
        ids = lax.broadcasted_iota(jnp.int32, (step, half), 1) + first
        return ids == code_all[span_of(n), 0:1].astype(jnp.int32)

    for n in range(tokens // step):
        span = pl.ds(n * step, step)
        scores = jnp.dot(h_all[span, :], w_all[...], preferred_element_type=f32)
        capped = softcap * jnp.tanh(scores * (1.0 / softcap))
        logits[span, :] = capped
        total = jnp.sum(jnp.exp(capped), axis=1, keepdims=True)
        hit_sum = jnp.sum(jnp.where(hits(n), capped, 0.0), axis=1, keepdims=True)
        turned = jnp.transpose(jnp.where(lax.rem(lanes, 8) < 4, total, hit_sum))
        stat_own[:, n * step:(n + 1) * step] = turned[0:8]

    def stat_copy(n):
        bb, vv, _ = peer(n)
        return copy(stat_own, stat_all.at[me], ss.at[n], sr.at[me], bb, vv)

    for n in range(len(peers)):
        stat_copy(n).start()
    for n in range(len(peers)):
        bb, vv, i = peer(n)
        copy(stat_own, stat_all.at[i], ss.at[n], sr.at[i], bb, vv).wait_recv()
    stats = stat_own[...]
    for n in range(len(peers)):
        stats = stats + stat_all[peer(n)[2]]

    loss = jnp.zeros((1, 1), f32)
    for n in range(tokens // step):
        span = pl.ds(n * step, step)
        weight = (code_all[span, 0:1] >= 0).astype(f32)
        back = jnp.transpose(jnp.concatenate([stats[:, n * step:(n + 1) * step]] * 16, axis=0))
        partition, target_logit = back[:, 0:1], back[:, 4:5]
        loss = loss + jnp.sum(weight * (jnp.log(partition) - target_logit), axis=0, keepdims=True)
        capped = logits[span, :]
        slope = 1.0 - (capped * (1.0 / softcap)) ** 2
        delta[span, :] = ((jnp.exp(capped) * (weight / partition) - jnp.where(hits(n), weight, 0.0)) * slope
                          ).astype(bf16)
    loss_own[...] = jnp.broadcast_to(loss, loss_own.shape)

    def loss_copy(k):
        return copy(loss_own, loss_all.at[b], ls.at[k - 1], lr.at[b], lax.rem(b + k, nb), v)

    def r_copy(zz, yy):
        i = zz * ny + yy
        return copy(grad_send.at[wrow(i)], r_in.at[z, y], rs.at[i], rr.at[b], i, v)

    def grad_share(span):
        return lax.dot_general(h_all[:, span], delta[...], (((0,), (0,)), ((), ())), preferred_element_type=f32)

    order = [lax.rem(z + k, nz) for k in range(1, nz)] + [z]
    slab = ny * cols
    if slab % 128 == 0:
        mine = y * cols
        for n in range(nz):
            zz = order[n]
            span = pl.ds(pl.multiple_of(zz * slab, 128), slab)
            share = grad_share(span)
            grad_send[span, :] = share.astype(bf16)
            if n == nz - 1:
                grad[...] = share
            for k in range(ny):
                if n < nz - 1 or k:
                    r_copy(zz, turn_y(k)).start()
    else:
        mine = b * cols
        wide = chunk_of(width, 256)

        def grad_step(j, carry):
            span = pl.ds(pl.multiple_of(j * wide, wide), wide)
            share = grad_share(span)
            grad[span, :] = share
            grad_send[span, :] = share.astype(bf16)
            return carry

        lax.fori_loop(0, width // wide, grad_step, 0)
        for n in range(nz):
            for k in range(ny):
                if n < nz - 1 or k:
                    r_copy(order[n], turn_y(k)).start()
    for k in range(1, nb):
        loss_copy(k).start()

    wide = chunk_of(width, 256)

    def part_step(j, carry):
        span = pl.ds(pl.multiple_of(j * wide, wide), wide)
        part[:, span] = lax.dot_general(
            delta[...], w_all[span, :], (((1,), (1,)), ((), ())), preferred_element_type=f32)
        return carry

    lax.fori_loop(0, width // wide, part_step, 0)

    def core_copy(kx, ky):
        i = turn_y(ky) * nv + turn_x(kx) * 2 + 1 - core
        return copy(part.at[hrow(i)], core_in.at[kx, ky], ds.at[kx, ky], dr.at[kx, ky], b, other)

    def x_copy(kx, ky):
        return copy(x_out.at[kx - 1, ky], x_in.at[kx - 1, ky], xs.at[kx, ky], xr.at[kx, ky],
                    b, turn_x(kx) * 2 + core)

    def y_copy(ky):
        return copy(y_out.at[ky - 1], y_in.at[ky - 1], ys.at[ky], yr.at[ky], z * ny + turn_y(ky), v)

    ways = [(kx % nx, ky % ny) for kx in range(1, nx + 1) for ky in range(1, ny + 1)]
    for kx, ky in ways:
        core_copy(kx, ky).start()
    hstep = 16

    def over_rows(start, body):
        def one(r, carry):
            body(pl.ds(pl.multiple_of(r * hstep, hstep), hstep),
                 pl.ds(pl.multiple_of(start + r * hstep, hstep), hstep))
            return carry

        lax.fori_loop(0, rows // hstep, one, 0)

    def start_of(kx, ky):
        return (turn_y(ky) * nv + turn_x(kx) * 2 + core) * rows

    for kx, ky in ways:
        core_copy(kx, ky).wait_recv()

        def core_sum(span, here):
            both = part[here, :] + core_in[kx, ky, span, :]
            if kx:
                x_out[kx - 1, ky, span, :] = both.astype(bf16)
            else:
                part[here, :] = both

        over_rows(start_of(kx, ky), core_sum)
        if kx:
            x_copy(kx, ky).start()

    for ky in [k % ny for k in range(1, ny + 1)]:
        for kx in range(1, nx):
            x_copy(kx, ky).wait_recv()

        def x_sum(span, here):
            total = part[here, :]
            for kx in range(1, nx):
                total = total + x_in[kx - 1, ky, span, :].astype(f32)
            if ky:
                y_out[ky - 1, span, :] = total.astype(bf16)
            else:
                hid_out[span, :] = total

        over_rows(start_of(0, ky), x_sum)
        if ky:
            y_copy(ky).start()

    cstep = chunk_of(cols, 64)

    def over_cols(body):
        def one(r, carry):
            body(pl.multiple_of(r * cstep, 16))
            return carry

        lax.fori_loop(0, cols // cstep, one, 0)

    def r_got(zz, yy):
        i = zz * ny + yy
        copy(grad_send.at[wrow(i)], r_in.at[zz, yy], rs.at[i], rr.at[i], i, v).wait_recv()

    for k in range(1, ny):
        r_got(z, turn_y(k))

    def first_sum(r):
        head_out[y, pl.ds(r, cstep), :] = grad[pl.ds(pl.multiple_of(mine + r, 16), cstep), :]
        for k in range(1, ny):
            head_out[turn_y(k), pl.ds(r, cstep), :] = r_in[z, turn_y(k), pl.ds(r, cstep), :].astype(f32)

    over_cols(first_sum)
    for n in range(1, nz):
        zz = lax.rem(z + nz - n, nz)
        for k in range(ny):
            r_got(zz, turn_y(k))
        if n == nz - 1:
            for ky in range(1, ny):
                y_copy(ky).wait_recv()

                def y_sum(span, here):
                    hid_out[span, :] += y_in[ky - 1, span, :].astype(f32)

                over_rows(0, y_sum)

        def more_sum(r):
            for k in range(ny):
                head_out[turn_y(k), pl.ds(r, cstep), :] += r_in[zz, turn_y(k), pl.ds(r, cstep), :].astype(f32)

        over_cols(more_sum)

    losses = loss_own[...]
    for k in range(1, nb):
        i = lax.rem(b + k, nb)
        copy(loss_own, loss_all.at[i], ls.at[k - 1], lr.at[i], i, v).wait_recv()
        losses = losses + loss_all[i]
    loss_out[...] = losses * (1.0 / (tokens * nb))

    for j in range(ny):
        yy = turn_y(j)
        pl.when(has_up)(lambda: w_z(z, yy, True, j == 0).wait_send())
        pl.when(has_down)(lambda: w_z(z, yy, False, j == 0).wait_send())
        for k in range(1, nz):
            @pl.when(z - k >= 0)
            def _():
                pl.when(has_up)(lambda: w_z(z - k, yy, True).wait_send())

            @pl.when(z + k < nz)
            def _():
                pl.when(has_down)(lambda: w_z(z + k, yy, False).wait_send())
    for k in range(1, ny):
        w_y(k).wait_send()
        h_y(k).wait_send()
        y_copy(k).wait_send()
    for k in range(1, nx):
        h_x(k).wait_send()
        for ky in range(1, ny):
            pl.when(core == 0)(lambda: h_xy(k, ky).wait_send())
            pl.when(core == 1)(lambda: h_yx(k, ky).wait_send())
    for kx, ky in ways:
        h_core(kx, ky).wait_send()
        core_copy(kx, ky).wait_send()
        if kx:
            x_copy(kx, ky).wait_send()
    for n in range(len(peers)):
        code_copy(n).wait_send()
        stat_copy(n).wait_send()
    for k in range(1, nb):
        loss_copy(k).wait_send()
    for n in range(nz):
        for k in range(ny):
            if n < nz - 1 or k:
                r_copy(order[n], turn_y(k)).wait_send()


def local(nb, nv, hidden, head_weight, targets, valid_mask):
    nx = nv // 2
    ny = nx if nx <= 2 and nb % nx == 0 else 1
    nz = nb // ny
    rows, width = hidden.shape
    entries, cols = head_weight.shape
    half = entries // ny
    group = ny * nv
    tokens = rows * group
    code = jnp.broadcast_to(jnp.where(valid_mask != 0, targets, -1).astype(f32)[None, :], (8, rows))
    weight = jnp.transpose(head_weight.reshape(ny, half, cols), (0, 2, 1))
    vm = pltpu.VMEM
    dma = pltpu.SemaphoreType.DMA
    slab = ny * cols
    ly, lx = max(ny - 1, 1), max(nx - 1, 1)
    buffers = [
        vm((tokens, width), bf16), vm((width, half), bf16), vm((group, 8, rows), f32), vm((tokens, 128), f32),
        vm((tokens, half), f32), vm((tokens, half), bf16),
        vm((8, tokens), f32), vm((group, 8, tokens), f32), vm((8, 128), f32), vm((nb, 8, 128), f32),
        vm((slab if slab % 128 == 0 else width, half), f32), vm((width, half), bf16), vm((nz, ny, cols, half), bf16),
        vm((tokens, width), f32), vm((nx, ny, rows, width), f32),
        vm((lx, ny, rows, width), bf16), vm((lx, ny, rows, width), bf16),
        vm((ly, rows, width), bf16), vm((ly, rows, width), bf16),
    ]
    sems = [
        dma((2,)), dma((nx + ny,)), dma((nx, ny)), dma((nx, ny)), dma((group,)), dma((nb,)), dma((nb,)),
        dma((ly,)), dma((nb,)), dma((group,)), dma((group,)), dma((group,)), dma((group,)), dma((nb,)), dma((nb,)),
        dma((nb,)), dma((nb,)), dma((nx, ny)), dma((nx, ny)), dma((nx, ny)), dma((nx, ny)), dma((ny,)), dma((ny,)),
    ]
    whole = pl.BlockSpec(memory_space=vm)
    head_t, hidden_grad, loss = pl.pallas_call(
        functools.partial(kernel, (nz, ny, nx, nv)),
        out_shape=(
            jax.ShapeDtypeStruct((ny, cols, half), f32),
            jax.ShapeDtypeStruct((rows, width), f32),
            jax.ShapeDtypeStruct((8, 128), f32),
        ),
        in_specs=[whole] * 3,
        out_specs=(whole,) * 3,
        scratch_shapes=buffers + sems,
        compiler_params=pltpu.CompilerParams(
            collective_id=0, has_side_effects=True, vmem_limit_bytes=67043328),
    )(hidden, weight, code)
    return jnp.transpose(head_t, (0, 2, 1)).reshape(entries, cols), hidden_grad, loss[0, 0]


def solution(mesh):
    placed = (
        P(("batch", "vocab"), None),
        P("vocab", "batch"),
        P(("batch", "vocab")),
        P(("batch", "vocab")),
    )
    return jax.shard_map(
        functools.partial(local, mesh.shape["batch"], mesh.shape["vocab"]),
        mesh=mesh,
        in_specs=placed,
        out_specs=(P("vocab", "batch"), P(("batch", "vocab"), None), P()),
        check_vma=False,
    )
```

```python
import functools

import jax
import jax.numpy as jnp
from jax import lax
from jax.experimental import pallas as pl
from jax.experimental.pallas import tpu as pltpu
from jax.sharding import PartitionSpec as P

softcap = 30.0
MESH = pl.DeviceIdType.MESH
f32, bf16 = jnp.float32, jnp.bfloat16


def chunk_of(length, most):
    return max(s for s in range(16, most + 1, 16) if length % s == 0)


def kernel(sizes, h_in, w_in, code_in, head_out, hid_out, loss_out, h_all, w_all, code_got, code_all,
           logits, delta, stat_own, stat_all, loss_own, loss_all, grad, grad_send, r_in,
           part, core_in, x_out, x_in, y_out, y_in, far_own, far_in, *sems):
    nz, ny, nx, nv = sizes
    (own_sem, hs, hf, hd, hr, ws_up, ws_dn, ws_y, wr, cs, cr, ss, sr, ls, lr,
     rs, rr, ds, dr, xs, xr, ys, yr, fs, fr) = sems
    nb = nz * ny
    rows, width = h_in.shape
    cols, half = w_in.shape[1:]
    group = ny * nv
    tokens = rows * group
    entries = ny * half
    b, v = lax.axis_index("batch"), lax.axis_index("vocab")
    z, y = lax.div(b, ny), lax.rem(b, ny)
    x, core = lax.div(v, 2), lax.rem(v, 2)
    other = x * 2 + 1 - core
    me = y * nv + v

    def at(bb, vv):
        return {"batch": bb, "vocab": vv}

    def copy(src, dst, send, recv, bb, vv):
        return pltpu.make_async_remote_copy(
            src_ref=src, dst_ref=dst, send_sem=send, recv_sem=recv, device_id=at(bb, vv), device_id_type=MESH)

    def hrow(i):
        return pl.ds(pl.multiple_of(i * rows, 16), rows)

    def wrow(i):
        return pl.ds(pl.multiple_of(i * cols, 16), cols)

    def turn_y(k):
        return lax.rem(y + k, ny)

    def turn_x(k):
        return lax.rem(x + k, nx)

    peers = [(k, j) for k in range(ny) for j in range(nv) if k or j]

    def peer(n):
        k, j = peers[n]
        return z * ny + turn_y(k), lax.rem(v + j, nv), turn_y(k) * nv + lax.rem(v + j, nv)

    barrier = pltpu.get_barrier_semaphore()
    for k in range(1, nb):
        pl.semaphore_signal(barrier, inc=1, device_id=at(lax.rem(b + k, nb), v), device_id_type=MESH)
    met = [n for n in range(len(peers)) if peers[n][1]]
    for n in met:
        bb, vv, _ = peer(n)
        pl.semaphore_signal(barrier, inc=1, device_id=at(bb, vv), device_id_type=MESH)
    pl.semaphore_wait(barrier, nb - 1 + len(met))

    def w_z(zz, yy, up, own=False):
        i = zz * ny + yy
        dst = w_all.at[wrow(i)]
        sem = (ws_up if up else ws_dn).at[i]
        return copy(w_in.at[y] if own else dst, dst, sem, wr.at[i], b + ny if up else b - ny, v)

    def w_y(k):
        return copy(w_in.at[turn_y(k)], w_all.at[wrow(b)], ws_y.at[k - 1], wr.at[b], z * ny + turn_y(k), v)

    def w_got(zz, yy):
        w_z(zz, yy, True).wait_recv()

    has_up, has_down = z + 1 < nz, z >= 1

    def h_send(n_src, sem, bb, vv, own=False):
        dst = h_all.at[hrow(n_src)]
        return copy(h_in if own else dst, dst, sem, hr.at[n_src], bb, vv)

    def h_x(k):
        return h_send(me, hs.at[k - 1], b, turn_x(k) * 2 + core, True)

    def h_y(k):
        return h_send(me, hs.at[nx + k - 1], z * ny + turn_y(k), v, True)

    def h_xy(kx, ky):
        return h_send(y * nv + turn_x(kx) * 2 + core, hf.at[kx, ky], z * ny + turn_y(ky), v)

    def h_yx(kx, ky):
        return h_send(turn_y(ky) * nv + v, hf.at[kx, ky], b, turn_x(kx) * 2 + core)

    def h_core(kx, ky):
        i = turn_y(ky) * nv + turn_x(kx) * 2 + core
        return h_send(i, hd.at[kx, ky], b, other, kx == 0 and ky == 0)

    def h_got(kx, ky, cc):
        i = turn_y(ky) * nv + turn_x(kx) * 2 + cc
        h_send(i, hd.at[kx, ky], b, other).wait_recv()

    def code_copy(n):
        bb, vv, _ = peer(n)
        return copy(code_in, code_got.at[me], cs.at[n], cr.at[me], bb, vv)

    for k in range(1, ny):
        w_y(k).start()
    pl.when(has_up)(lambda: w_z(z, y, True, True).start())
    pl.when(has_down)(lambda: w_z(z, y, False, True).start())
    for k in range(1, nx):
        h_x(k).start()
    for k in range(1, ny):
        h_y(k).start()
    for n in range(len(peers)):
        code_copy(n).start()
    h_core(0, 0).start()
    local = [
        pltpu.make_async_copy(w_in.at[y], w_all.at[wrow(b)], own_sem.at[0]),
        pltpu.make_async_copy(h_in, h_all.at[hrow(me)], own_sem.at[1]),
    ]
    for one in local:
        one.start()

    for k in range(1, ny):
        w_got(z, turn_y(k))
        pl.when(has_up)(lambda: w_z(z, turn_y(k), True).start())
        pl.when(has_down)(lambda: w_z(z, turn_y(k), False).start())

    def h_pass():
        for kx in range(1, nx):
            h_got(kx, 0, core)
            for ky in range(1, ny):
                pl.when(core == 0)(lambda: h_xy(kx, ky).start())
            h_core(kx, 0).start()
        for ky in range(1, ny):
            h_got(0, ky, core)
            for kx in range(1, nx):
                pl.when(core == 1)(lambda: h_yx(kx, ky).start())
            h_core(0, ky).start()

    def h_rest():
        for kx in range(1, nx):
            for ky in range(1, ny):
                h_got(kx, ky, core)
                h_core(kx, ky).start()

    for k in range(1, nz):
        for j in range(ny):
            yy = turn_y(j)

            @pl.when(z - k >= 0)
            def _():
                w_got(z - k, yy)
                pl.when(has_up)(lambda: w_z(z - k, yy, True).start())

            @pl.when(z + k < nz)
            def _():
                w_got(z + k, yy)
                pl.when(has_down)(lambda: w_z(z + k, yy, False).start())
        if k == 1:
            h_pass()
        if k == min(2, nz - 1):
            h_rest()

    for one in local:
        one.wait()
    for kx in range(nx):
        for ky in range(ny):
            h_got(kx, ky, 1 - core)
    code_got[me] = code_in[...]
    for n in range(len(peers)):
        bb, vv, i = peer(n)
        copy(code_in, code_got.at[i], cs.at[n], cr.at[i], bb, vv).wait_recv()
    for i in range(group):
        code_all[i * rows:(i + 1) * rows, :] = jnp.transpose(jnp.concatenate([code_got[i]] * 16, axis=0))

    step = chunk_of(tokens, 256)
    lanes = lax.broadcasted_iota(jnp.int32, (step, 128), 1)
    first = v * entries + y * half

    def span_of(n):
        return pl.ds(pl.multiple_of(n * step, step), step)

    def hits(n):
        ids = lax.broadcasted_iota(jnp.int32, (step, half), 1) + first
        return ids == code_all[span_of(n), 0:1].astype(jnp.int32)

    for n in range(tokens // step):
        span = pl.ds(n * step, step)
        scores = jnp.dot(h_all[span, :], w_all[...], preferred_element_type=f32)
        capped = softcap * jnp.tanh(scores * (1.0 / softcap))
        logits[span, :] = capped
        total = jnp.sum(jnp.exp(capped), axis=1, keepdims=True)
        hit_sum = jnp.sum(jnp.where(hits(n), capped, 0.0), axis=1, keepdims=True)
        turned = jnp.transpose(jnp.where(lax.rem(lanes, 8) < 4, total, hit_sum))
        stat_own[:, n * step:(n + 1) * step] = turned[0:8]

    def stat_copy(n):
        bb, vv, _ = peer(n)
        return copy(stat_own, stat_all.at[me], ss.at[n], sr.at[me], bb, vv)

    for n in range(len(peers)):
        stat_copy(n).start()
    for n in range(len(peers)):
        bb, vv, i = peer(n)
        copy(stat_own, stat_all.at[i], ss.at[n], sr.at[i], bb, vv).wait_recv()
    stats = stat_own[...]
    for n in range(len(peers)):
        stats = stats + stat_all[peer(n)[2]]

    loss = jnp.zeros((1, 1), f32)
    for n in range(tokens // step):
        span = pl.ds(n * step, step)
        weight = (code_all[span, 0:1] >= 0).astype(f32)
        back = jnp.transpose(jnp.concatenate([stats[:, n * step:(n + 1) * step]] * 16, axis=0))
        partition, target_logit = back[:, 0:1], back[:, 4:5]
        loss = loss + jnp.sum(weight * (jnp.log(partition) - target_logit), axis=0, keepdims=True)
        capped = logits[span, :]
        slope = 1.0 - (capped * (1.0 / softcap)) ** 2
        delta[span, :] = ((jnp.exp(capped) * (weight / partition) - jnp.where(hits(n), weight, 0.0)) * slope
                          ).astype(bf16)
    loss_own[...] = jnp.broadcast_to(loss, loss_own.shape)

    def loss_copy(k):
        return copy(loss_own, loss_all.at[b], ls.at[k - 1], lr.at[b], lax.rem(b + k, nb), v)

    def r_copy(zz, yy):
        i = zz * ny + yy
        return copy(grad_send.at[wrow(i)], r_in.at[z, y], rs.at[i], rr.at[b], i, v)

    def grad_share(span):
        return lax.dot_general(h_all[:, span], delta[...], (((0,), (0,)), ((), ())), preferred_element_type=f32)

    slab = ny * cols
    relay = nz == 4 and slab % 128 == 0
    turn = jnp.where(z * 2 >= nz, 1, nz - 1)
    order = [lax.rem(z + turn * k, nz) for k in range(1, nz)] + [z]
    at_end = (z == 0) | (z == nz - 1)
    far = jnp.where(z * 2 >= nz, 0, nz - 1)
    near = jnp.where(z * 2 >= nz, z - 1, z + 1)

    def far_copy(yy):
        return copy(grad_send.at[wrow(far * ny + yy)], far_in.at[yy], fs.at[yy], fr.at[yy], near * ny + y, v)

    def direct(zz):
        return jnp.logical_not(at_end & (zz == far))
    if slab % 128 == 0:
        mine = y * cols
        for n in range(nz):
            zz = order[n]
            span = pl.ds(pl.multiple_of(zz * slab, 128), slab)
            share = grad_share(span)
            held = relay and n == 1
            if n == nz - 1:
                grad[...] = share
            if held:
                @pl.when(jnp.logical_not(at_end))
                def _():
                    far_own[...] = share

                @pl.when(at_end)
                def _():
                    grad_send[span, :] = share.astype(bf16)
                    for k in range(ny):
                        r_copy(zz, turn_y(k)).start()
            else:
                grad_send[span, :] = share.astype(bf16)
                for k in range(ny):
                    yy = turn_y(k)
                    if relay and n == 0:
                        pl.when(at_end)(lambda: far_copy(yy).start())
                        pl.when(jnp.logical_not(at_end))(lambda: r_copy(zz, yy).start())
                    elif n < nz - 1 or k:
                        r_copy(zz, yy).start()
    else:
        mine = b * cols
        wide = chunk_of(width, 256)

        def grad_step(j, carry):
            span = pl.ds(pl.multiple_of(j * wide, wide), wide)
            share = grad_share(span)
            grad[span, :] = share
            grad_send[span, :] = share.astype(bf16)
            return carry

        lax.fori_loop(0, width // wide, grad_step, 0)
        for n in range(nz):
            for k in range(ny):
                if n < nz - 1 or k:
                    r_copy(order[n], turn_y(k)).start()
    for k in range(1, nb):
        loss_copy(k).start()

    wide = chunk_of(width, 256)

    def part_step(j, carry):
        span = pl.ds(pl.multiple_of(j * wide, wide), wide)
        part[:, span] = lax.dot_general(
            delta[...], w_all[span, :], (((1,), (1,)), ((), ())), preferred_element_type=f32)
        return carry

    lax.fori_loop(0, width // wide, part_step, 0)

    def core_copy(kx, ky):
        i = turn_y(ky) * nv + turn_x(kx) * 2 + 1 - core
        return copy(part.at[hrow(i)], core_in.at[kx, ky], ds.at[kx, ky], dr.at[kx, ky], b, other)

    def x_copy(kx, ky):
        return copy(x_out.at[kx - 1, ky], x_in.at[kx - 1, ky], xs.at[kx, ky], xr.at[kx, ky],
                    b, turn_x(kx) * 2 + core)

    def y_copy(ky):
        return copy(y_out.at[ky - 1], y_in.at[ky - 1], ys.at[ky], yr.at[ky], z * ny + turn_y(ky), v)

    ways = [(kx % nx, ky % ny) for kx in range(1, nx + 1) for ky in range(1, ny + 1)]
    for kx, ky in ways:
        core_copy(kx, ky).start()
    hstep = 16

    def over_rows(start, body):
        def one(r, carry):
            body(pl.ds(pl.multiple_of(r * hstep, hstep), hstep),
                 pl.ds(pl.multiple_of(start + r * hstep, hstep), hstep))
            return carry

        lax.fori_loop(0, rows // hstep, one, 0)

    def start_of(kx, ky):
        return (turn_y(ky) * nv + turn_x(kx) * 2 + core) * rows

    for kx, ky in ways:
        core_copy(kx, ky).wait_recv()

        def core_sum(span, here):
            both = part[here, :] + core_in[kx, ky, span, :]
            if kx:
                x_out[kx - 1, ky, span, :] = both.astype(bf16)
            else:
                part[here, :] = both

        over_rows(start_of(kx, ky), core_sum)
        if kx:
            x_copy(kx, ky).start()

    cstep = chunk_of(cols, 64)

    def over_cols(body):
        def one(r, carry):
            body(pl.multiple_of(r * cstep, 16))
            return carry

        lax.fori_loop(0, cols // cstep, one, 0)

    if relay:
        @pl.when(jnp.logical_not(at_end))
        def _():
            for k in range(ny):
                yy = turn_y(k)
                far_copy(yy).wait_recv()

                def far_sum(r):
                    here = pl.ds(pl.multiple_of(yy * cols + r, 16), cstep)
                    there = pl.ds(pl.multiple_of((far * ny + yy) * cols + r, 16), cstep)
                    grad_send[there, :] = (far_own[here, :] + far_in[yy, pl.ds(r, cstep), :].astype(f32)).astype(bf16)

                over_cols(far_sum)
                r_copy(far, yy).start()

    for ky in [k % ny for k in range(1, ny + 1)]:
        for kx in range(1, nx):
            x_copy(kx, ky).wait_recv()

        def x_sum(span, here):
            total = part[here, :]
            for kx in range(1, nx):
                total = total + x_in[kx - 1, ky, span, :].astype(f32)
            if ky:
                y_out[ky - 1, span, :] = total.astype(bf16)
            else:
                hid_out[span, :] = total

        over_rows(start_of(0, ky), x_sum)
        if ky:
            y_copy(ky).start()

    def r_got(zz, yy):
        i = zz * ny + yy
        copy(grad_send.at[wrow(i)], r_in.at[zz, yy], rs.at[i], rr.at[i], i, v).wait_recv()

    for k in range(1, ny):
        r_got(z, turn_y(k))

    def first_sum(r):
        head_out[y, pl.ds(r, cstep), :] = grad[pl.ds(pl.multiple_of(mine + r, 16), cstep), :]
        for k in range(1, ny):
            head_out[turn_y(k), pl.ds(r, cstep), :] = r_in[z, turn_y(k), pl.ds(r, cstep), :].astype(f32)

    over_cols(first_sum)
    hops = [jnp.where(z * 2 >= nz, lax.rem(z + nz - n, nz), lax.rem(z + n, nz)) for n in range(1, nz)]
    for n in range(1, nz):
        zz = hops[n - 1]
        if n == nz - 1:
            for ky in range(1, ny):
                y_copy(ky).wait_recv()

                def y_sum(span, here):
                    hid_out[span, :] += y_in[ky - 1, span, :].astype(f32)

                over_rows(0, y_sum)

        def more_sum(r):
            for k in range(ny):
                head_out[turn_y(k), pl.ds(r, cstep), :] += r_in[zz, turn_y(k), pl.ds(r, cstep), :].astype(f32)

        def arrived():
            for k in range(ny):
                r_got(zz, turn_y(k))
            over_cols(more_sum)

        if relay:
            pl.when(direct(zz))(arrived)
        else:
            arrived()

    losses = loss_own[...]
    for k in range(1, nb):
        i = lax.rem(b + k, nb)
        copy(loss_own, loss_all.at[i], ls.at[k - 1], lr.at[i], i, v).wait_recv()
        losses = losses + loss_all[i]
    loss_out[...] = losses * (1.0 / (tokens * nb))

    for j in range(ny):
        yy = turn_y(j)
        pl.when(has_up)(lambda: w_z(z, yy, True, j == 0).wait_send())
        pl.when(has_down)(lambda: w_z(z, yy, False, j == 0).wait_send())
        for k in range(1, nz):
            @pl.when(z - k >= 0)
            def _():
                pl.when(has_up)(lambda: w_z(z - k, yy, True).wait_send())

            @pl.when(z + k < nz)
            def _():
                pl.when(has_down)(lambda: w_z(z + k, yy, False).wait_send())
    for k in range(1, ny):
        w_y(k).wait_send()
        h_y(k).wait_send()
        y_copy(k).wait_send()
    for k in range(1, nx):
        h_x(k).wait_send()
        for ky in range(1, ny):
            pl.when(core == 0)(lambda: h_xy(k, ky).wait_send())
            pl.when(core == 1)(lambda: h_yx(k, ky).wait_send())
    for kx, ky in ways:
        h_core(kx, ky).wait_send()
        core_copy(kx, ky).wait_send()
        if kx:
            x_copy(kx, ky).wait_send()
    for n in range(len(peers)):
        code_copy(n).wait_send()
        stat_copy(n).wait_send()
    for k in range(1, nb):
        loss_copy(k).wait_send()
    for n in range(nz):
        for k in range(ny):
            yy = turn_y(k)
            if relay and n == 0:
                pl.when(at_end)(lambda: far_copy(yy).wait_send())
                pl.when(jnp.logical_not(at_end))(lambda: r_copy(order[n], yy).wait_send())
            elif n < nz - 1 or k:
                r_copy(order[n], yy).wait_send()


def local(nb, nv, hidden, head_weight, targets, valid_mask):
    nx = nv // 2
    ny = nx if nx <= 2 and nb % nx == 0 else 1
    nz = nb // ny
    rows, width = hidden.shape
    entries, cols = head_weight.shape
    half = entries // ny
    group = ny * nv
    tokens = rows * group
    code = jnp.broadcast_to(jnp.where(valid_mask != 0, targets, -1).astype(f32)[None, :], (8, rows))
    weight = jnp.transpose(head_weight.reshape(ny, half, cols), (0, 2, 1))
    vm = pltpu.VMEM
    dma = pltpu.SemaphoreType.DMA
    slab = ny * cols
    ly, lx = max(ny - 1, 1), max(nx - 1, 1)
    buffers = [
        vm((tokens, width), bf16), vm((width, half), bf16), vm((group, 8, rows), f32), vm((tokens, 128), f32),
        vm((tokens, half), f32), vm((tokens, half), bf16),
        vm((8, tokens), f32), vm((group, 8, tokens), f32), vm((8, 128), f32), vm((nb, 8, 128), f32),
        vm((slab if slab % 128 == 0 else width, half), f32), vm((width, half), bf16), vm((nz, ny, cols, half), bf16),
        vm((tokens, width), f32), vm((nx, ny, rows, width), f32),
        vm((lx, ny, rows, width), bf16), vm((lx, ny, rows, width), bf16),
        vm((ly, rows, width), bf16), vm((ly, rows, width), bf16),
        vm((slab if nz == 4 else 16, half), f32), vm((ny, cols if nz == 4 else 16, half), bf16),
    ]
    sems = [
        dma((2,)), dma((nx + ny,)), dma((nx, ny)), dma((nx, ny)), dma((group,)), dma((nb,)), dma((nb,)),
        dma((ly,)), dma((nb,)), dma((group,)), dma((group,)), dma((group,)), dma((group,)), dma((nb,)), dma((nb,)),
        dma((nb,)), dma((nb,)), dma((nx, ny)), dma((nx, ny)), dma((nx, ny)), dma((nx, ny)), dma((ny,)), dma((ny,)),
        dma((ny,)), dma((ny,)),
    ]
    whole = pl.BlockSpec(memory_space=vm)
    head_t, hidden_grad, loss = pl.pallas_call(
        functools.partial(kernel, (nz, ny, nx, nv)),
        out_shape=(
            jax.ShapeDtypeStruct((ny, cols, half), f32),
            jax.ShapeDtypeStruct((rows, width), f32),
            jax.ShapeDtypeStruct((8, 128), f32),
        ),
        in_specs=[whole] * 3,
        out_specs=(whole,) * 3,
        scratch_shapes=buffers + sems,
        compiler_params=pltpu.CompilerParams(
            collective_id=0, has_side_effects=True, vmem_limit_bytes=67043328),
    )(hidden, weight, code)
    return jnp.transpose(head_t, (0, 2, 1)).reshape(entries, cols), hidden_grad, loss[0, 0]


def solution(mesh):
    placed = (
        P(("batch", "vocab"), None),
        P("vocab", "batch"),
        P(("batch", "vocab")),
        P(("batch", "vocab")),
    )
    return jax.shard_map(
        functools.partial(local, mesh.shape["batch"], mesh.shape["vocab"]),
        mesh=mesh,
        in_specs=placed,
        out_specs=(P("vocab", "batch"), P(("batch", "vocab"), None), P()),
        check_vma=False,
    )
```
